32 devices in a mesh: dp: 4 (over y, x), ctx: 8 (over z, core).
Axes of the slice: x: 2, y: 2, z: 4, core: 2. Of those that a mesh axis runs over, the one named last changes fastest.
Arguments:
- layer_input: bfloat16 [4, 1024, 7168], P(None, 'ctx', 'dp'), may hold values from -6 to 6
- kv_latent: bfloat16 [4, 1024, 512], P('dp', 'ctx'), may hold values from -8 to 8
- key_rope: bfloat16 [4, 1024, 64], P('dp', 'ctx'), may hold values from -6 to 6
- q_latent: bfloat16 [4, 1024, 8, 512], P('dp', 'ctx'), may hold values from -60 to 60
- q_rope: bfloat16 [4, 1024, 8, 64], P('dp', 'ctx'), may hold values from -3 to 3
- saved_output: bfloat16 [4, 1024, 8, 512], P('dp', 'ctx'), may hold values from -4 to 4
- w_uv: bfloat16 [512, 1024], replicated, may hold values from -0.25 to 0.25
- d_out: bfloat16 [4, 1024, 1024], P('dp', 'ctx'), may hold values from -6 to 6
- blocks: int32 [16], replicated, may hold values from 0 to 15, each once
Outputs:
- d_q_latent: bfloat16 [4, 1024, 8, 512], P('dp', 'ctx')
- d_q_rope: bfloat16 [4, 1024, 8, 64], P('dp', 'ctx')
- d_kv_latent: bfloat16 [4, 1024, 512], P('dp', 'ctx')
- d_key_rope: bfloat16 [4, 1024, 64], P('dp', 'ctx')
- grad_w_down: float32 [7168, 576], P(('dp', 'ctx'))
- grad_w_uv: float32 [512, 1024], P(('dp', 'ctx'))
The draws below stay inside these ranges and needn't reach their ends.
Inputs may be any that keep to these rules, and one draw needn't show every extreme that they name: A permutation: blocks[k] is the position block of rows k * 64 to (k + 1) * 64 - 1 of every sequence.
All inputs are finite; a program needn't handle non-finite values.
Results may differ from the reference program's by a relative error of at most 0.028.
Values may be sent and summed in bfloat16 or wider, within the bound.
A program may use at most 128 MiB of HBM per device.

```python
import functools
import math
import jax
import jax.numpy as jnp
from jax import lax

D = 7168
KVL = 512
ROPE = 64
VHEAD = 128
HEADS = 8
TOK_DEV = 128
SEQ = 1024
N_DP = 4
N_CTX = 8


def base_latent(key):
    return jnp.clip(jax.random.normal(jax.random.fold_in(key, 7), (N_DP, SEQ, KVL), jnp.float32), -6.0, 6.0)


def draw_kv_latent(key, part):
    latent = base_latent(key)
    return latent.astype(jnp.bfloat16)


def draw_q_latent(key, part):
    queries = 0.5 * jnp.clip(jax.random.normal(jax.random.fold_in(key, 9), (N_DP, SEQ, HEADS, KVL), jnp.float32), -6.0, 6.0)
    return queries.astype(jnp.bfloat16)


def strengthened(drawn, own_key, source, target, blocks, factor):
    owner, partner = [(jnp.arange(drawn.shape[axis_at]) // (drawn.shape[axis_at] // blocks)).reshape([-1 if axis == axis_at else 1 for axis in range(drawn.ndim)]) for axis_at in (source, target)]
    chosen = jax.random.permutation(own_key, blocks)[partner]
    strong = (owner == chosen) | (owner == (partner + blocks // 2) % blocks)
    return jnp.where(strong, factor * drawn, drawn)


def block_levels(rng, shape, shards, smallest, high):
    factor_of, own = 1.0, jax.random.fold_in(rng, 6)
    for dim, blocks in shards:
        steps = jnp.exp(jax.random.uniform(jax.random.fold_in(own, dim), (blocks,), jnp.float32, smallest / len(shards), high / len(shards)))
        factor_of = factor_of * jnp.repeat(steps, shape[dim] // blocks).reshape([-1 if axis == dim else 1 for axis in range(len(shape))])
    return factor_of


def scatter_about(stream_key, shape, width, limit, split=(), kind=jnp.bfloat16):
    level = block_levels(stream_key, shape, split, -0.22, 0.18) if split else 1.0
    values = jax.random.normal(stream_key, shape, jnp.float32) * width * level
    return jnp.minimum(jnp.maximum(values, -limit), limit).astype(kind)


def bell_draw_with(key, shape, spread, most, split, heavy, kind=jnp.bfloat16):
    drawn = spread * jax.random.normal(key, shape, jnp.float32)
    if split:
        drawn = drawn * block_levels(key, shape, split, -0.22, 0.18)
    return jnp.clip(strengthened(drawn, jax.random.fold_in(key, 3), *heavy), -most, most).astype(kind)


def setup_inputs(seed: int = 0) -> dict:
    splits = jax.random.split(jax.random.key(seed), 10)
    return {
        "layer_input": bell_draw_with(splits[0], (N_DP, SEQ, D), 1.0, 6.0, ((1, 8), (2, 4)), (1, 2, 8, 2.0)),
        "kv_latent": draw_kv_latent(jax.random.fold_in(splits[9], 71), 0),
        "key_rope": scatter_about(splits[2], (N_DP, SEQ, ROPE), 1.0, 6.0, ((0, 4), (1, 8))),
        "q_latent": draw_q_latent(jax.random.fold_in(splits[9], 71), 0),
        "q_rope": scatter_about(splits[4], (N_DP, SEQ, HEADS, ROPE), 0.5, 3.0, ((0, 4), (1, 8))),
        "saved_output": scatter_about(splits[5], (N_DP, SEQ, HEADS, KVL), 0.5, 4.0, ((0, 4), (1, 8))),
        "w_uv": scatter_about(splits[6], (KVL, HEADS * VHEAD), KVL ** -0.5, 0.25),
        "d_out": scatter_about(splits[7], (N_DP, SEQ, HEADS * VHEAD), 1.0, 6.0, ((0, 4), (1, 8))),
        "blocks": jax.random.permutation(splits[8], 2 * N_CTX).astype(jnp.int32),
    }


softmax_scale = 1.0 / math.sqrt(192.0)

def group_grads(carry, group, latent_keys, rope_keys, positions, value_weight):
    term_lat, term_rope, value_total = carry
    query_lat, query_rope, saved_rows, grad_out, query_pos = group
    wide = jnp.float32
    keys_wide = latent_keys.astype(wide)
    rope_wide = rope_keys.astype(wide)
    scores = jnp.einsum('thk,jk->thj', query_lat.astype(wide), keys_wide)
    scores = scores + jnp.einsum('thr,jr->thj', query_rope.astype(wide), rope_wide)
    scores = scores * softmax_scale
    visible = positions[None, None, :] <= query_pos[:, None, None]
    masked = jnp.where(visible, scores, -jnp.inf)
    row_max = lax.optimization_barrier(jnp.max(masked, axis=2, keepdims=True))
    log_total = row_max + jnp.log(lax.optimization_barrier(jnp.sum(jnp.exp(masked - row_max), axis=2, keepdims=True)))
    probs = jnp.exp(masked - log_total)
    probs_low = probs.astype(jnp.bfloat16)
    grad_lat = jnp.einsum('thv,khv->thk', grad_out.astype(wide), value_weight.astype(wide)).astype(jnp.bfloat16)
    delta = lax.optimization_barrier(jnp.sum(grad_lat.astype(wide) * saved_rows.astype(wide), axis=2, keepdims=True))
    grad_prob = jnp.einsum('thk,jk->thj', grad_lat.astype(wide), keys_wide)
    grad_score = (probs * (grad_prob - delta)).astype(jnp.bfloat16)
    score_wide = grad_score.astype(wide)
    dq_lat = (softmax_scale * jnp.einsum('thj,jk->thk', score_wide, keys_wide)).astype(jnp.bfloat16)
    dq_rope = (softmax_scale * jnp.einsum('thj,jr->thr', score_wide, rope_wide)).astype(jnp.bfloat16)
    part_lat = jnp.einsum('thj,thk->jk', probs_low.astype(wide), grad_lat.astype(wide))
    part_lat = part_lat + softmax_scale * jnp.einsum('thj,thk->jk', score_wide, query_lat.astype(wide))
    part_rope = softmax_scale * jnp.einsum('thj,thr->jr', score_wide, query_rope.astype(wide))
    term_lat = term_lat + lax.optimization_barrier(part_lat.astype(jnp.bfloat16)).astype(wide)
    term_rope = term_rope + lax.optimization_barrier(part_rope.astype(jnp.bfloat16)).astype(wide)
    value_total = value_total + jnp.einsum('thk,thv->khv', saved_rows.astype(wide), grad_out.astype(wide))
    return ((term_lat, term_rope, value_total), (dq_lat, dq_rope))

def reference(layer_input, kv_latent, key_rope, q_latent, q_rope, saved_output, w_uv, d_out, blocks):
    half_rows = TOK_DEV // 2
    row_ids = jnp.arange(SEQ, dtype=jnp.int32)
    positions = (blocks[row_ids // half_rows] * half_rows + row_ids % half_rows).astype(jnp.int32)
    value_weight = w_uv.reshape(KVL, HEADS, VHEAD)
    query_pos = positions.reshape(N_CTX, TOK_DEV)
    value_total = jnp.zeros((KVL, HEADS, VHEAD), jnp.float32)
    down_total = jnp.zeros((D, KVL + ROPE), jnp.float32)
    dql_list, dqr_list, dkv_list, dkr_list = ([], [], [], [])
    for seq_index in range(N_DP):
        groups = (q_latent[seq_index].reshape(N_CTX, TOK_DEV, HEADS, KVL), q_rope[seq_index].reshape(N_CTX, TOK_DEV, HEADS, ROPE), saved_output[seq_index].reshape(N_CTX, TOK_DEV, HEADS, KVL), d_out[seq_index].reshape(N_CTX, TOK_DEV, HEADS, VHEAD), query_pos)
        step_fn = functools.partial(group_grads, latent_keys=kv_latent[seq_index], rope_keys=key_rope[seq_index], positions=positions, value_weight=value_weight)
        start = (jnp.zeros((SEQ, KVL), jnp.float32), jnp.zeros((SEQ, ROPE), jnp.float32), value_total)
        (term_lat, term_rope, value_total), (dq_lat, dq_rope) = lax.scan(step_fn, start, groups)
        dkv_low = term_lat.astype(jnp.bfloat16)
        dkr_low = term_rope.astype(jnp.bfloat16)
        joined = jnp.concatenate([dkv_low, dkr_low], axis=1)
        down_total = down_total + jnp.dot(layer_input[seq_index].T, joined, preferred_element_type=jnp.float32)
        dql_list.append(dq_lat.reshape(SEQ, HEADS, KVL))
        dqr_list.append(dq_rope.reshape(SEQ, HEADS, ROPE))
        dkv_list.append(dkv_low)
        dkr_list.append(dkr_low)
    return (jnp.stack(dql_list), jnp.stack(dqr_list), jnp.stack(dkv_list), jnp.stack(dkr_list), down_total, value_total.reshape(KVL, HEADS * VHEAD))
```

```python
import functools
import math

import jax
import jax.numpy as jnp
from jax import lax
from jax.experimental import pallas as pl
from jax.experimental.pallas import tpu as pltpu
from jax.sharding import PartitionSpec as P

softmax_scale = 1.0 / math.sqrt(192.0)
wide = jnp.float32
low = jnp.bfloat16
MESH = pl.DeviceIdType.MESH
VMEM_LIMIT = 62 * 1024 * 1024


def dot(a, b, ca, cb):
    return lax.dot_general(a, b, (((ca,), (cb,)), ((), ())), preferred_element_type=wide)


def greet(peers):
    barrier = pltpu.get_barrier_semaphore()
    for peer in peers:
        pl.semaphore_signal(barrier, inc=1, device_id=peer, device_id_type=MESH)
    pl.semaphore_wait(barrier, len(peers))


def remote(src, dst, send, recv, peer):
    return pltpu.make_async_remote_copy(
        src_ref=src, dst_ref=dst, send_sem=send, recv_sem=recv, device_id=peer, device_id_type=MESH
    )


def gather_kernel(
    n_dp, n_ctx,
    key_ref, spread_ref, weight_ref, saved_ref,
    keys_ref, grad_ref, delta_ref, value_ref,
    parts, landed, key_send, key_recv, pair_send, pair_recv, val_send, val_recv,
):
    dp, ctx = lax.axis_index("dp"), lax.axis_index("ctx")
    n_z = n_ctx // 2
    z, core = ctx // 2, ctx % 2
    tokens = key_ref.shape[0]
    partner = (dp, z * 2 + (1 - core))
    z_peer = lambda k: (dp, lax.rem(z + k, n_z) * 2 + core)
    dp_peer = lambda k: (lax.rem(dp + k, n_dp), ctx)
    greet(
        [partner]
        + [z_peer(k) for k in range(1, n_z)]
        + [dp_peer(k) for k in range(1, n_dp)]
    )

    def rows_of(index):
        return keys_ref.at[pl.ds(pl.multiple_of(index * tokens, tokens), tokens)]

    sends = []
    for k in range(1, n_z):
        copy = remote(key_ref, rows_of(ctx), key_send.at[k], key_recv.at[k], z_peer(k))
        copy.start()
        sends.append(copy)
    pair = remote(key_ref, rows_of(ctx), pair_send.at[0], pair_recv.at[0], partner)
    pair.start()
    keys_ref[pl.ds(pl.multiple_of(ctx * tokens, tokens), tokens), :] = key_ref[...]

    share = parts.shape[1]
    value = dot(saved_ref[...], spread_ref[...], 0, 0).astype(low)
    for d in range(n_dp):
        parts[d] = value[d * share : (d + 1) * share]
    value_copies = []
    for k in range(1, n_dp):
        copy = remote(
            parts.at[lax.rem(dp + k, n_dp)], landed.at[k], val_send.at[k], val_recv.at[k], dp_peer(k)
        )
        copy.start()
        value_copies.append(copy)

    rows = spread_ref.shape[0]
    tile = min(256, rows)
    for start in range(0, rows, tile):
        grad = dot(spread_ref[start : start + tile], weight_ref[...], 1, 1).astype(low)
        grad_ref[start : start + tile, :] = grad
        prod = grad.astype(wide) * saved_ref[start : start + tile].astype(wide)
        part = prod[:, :128]
        for lane in range(128, prod.shape[1], 128):
            part = part + prod[:, lane : lane + 128]
        delta_ref[:, start : start + tile] = jnp.sum(part.T, axis=0, keepdims=True)

    passes = []
    for k in range(1, n_z):
        owner = lax.rem(z + n_z - k, n_z) * 2 + core
        remote(key_ref, rows_of(owner), key_send.at[k], key_recv.at[k], z_peer(k)).wait_recv()
        copy = remote(rows_of(owner), rows_of(owner), pair_send.at[k], pair_recv.at[k], partner)
        copy.start()
        passes.append(copy)
    total = parts[dp].astype(wide)
    for k in range(1, n_dp):
        value_copies[k - 1].wait_recv()
        total = total + landed[k].astype(wide)
    total = total.astype(low)
    piece = value_ref.shape[1]
    for c in range(n_ctx):
        value_ref[c] = total[c * piece : (c + 1) * piece]
    for k in range(n_z):
        owner = lax.rem(z + n_z - k, n_z) * 2 + (1 - core)
        remote(rows_of(owner), rows_of(owner), pair_send.at[k], pair_recv.at[k], partner).wait_recv()
    for copy in sends + [pair] + passes + value_copies:
        copy.wait_send()


def attend_kernel(
    keys_ref, posk_ref, posq_ref, delta_ref, ql_ref, qr_ref, grad_ref,
    dql_ref, dqr_ref, term_ref, total,
):
    step = pl.program_id(0)
    latent = ql_ref.shape[1]
    key_lat = keys_ref[:, :latent]
    key_rope = keys_ref[:, latent:]
    ql, qr, grad = ql_ref[...], qr_ref[...], grad_ref[...]
    scores = (dot(key_lat, ql, 1, 1) + dot(key_rope, qr, 1, 1)) * softmax_scale
    scores = jnp.where(posk_ref[...] <= posq_ref[...], scores, -jnp.inf)
    top = jnp.max(scores, axis=0, keepdims=True)
    expo = jnp.exp(scores - top)
    probs = expo * (1.0 / jnp.sum(expo, axis=0, keepdims=True))
    grad_prob = dot(key_lat, grad, 1, 1)
    slope = (probs * (grad_prob - delta_ref[...])).astype(low)
    dql_ref[...] = (softmax_scale * dot(slope, key_lat, 0, 0)).astype(low)
    dqr_ref[...] = (softmax_scale * dot(slope, key_rope, 0, 0)).astype(low)
    lat = dot(probs.astype(low), grad, 1, 0) + softmax_scale * dot(slope, ql, 1, 0)
    rope = softmax_scale * dot(slope, qr, 1, 0)

    @pl.when(step == 0)
    def _():
        total[:, :latent] = lat
        total[:, latent:] = rope

    @pl.when(step > 0)
    def _():
        total[:, :latent] += lat
        total[:, latent:] += rope

    @pl.when(step == pl.num_programs(0) - 1)
    def _():
        term_ref[...] = total[...].astype(low)


def reduce_kernel(
    n_dp, n_ctx,
    term_ref, layer_ref, value_ref,
    joined_ref, down_ref, uv_ref,
    turned, pair_in, pair_sum, z_in, blocks_in, down_out, down_own, down_in, down_sum, down_z, value_in,
    a_send, a_recv, b_send, b_recv, c_send, c_recv, d_send, d_recv, e_send, e_recv, f_send, f_recv,
):
    dp, ctx = lax.axis_index("dp"), lax.axis_index("ctx")
    n_z = n_ctx // 2
    z, core = ctx // 2, ctx % 2
    tokens = joined_ref.shape[0]
    other = 1 - core
    partner = (dp, z * 2 + other)
    chip = lambda k: lax.rem(z + k, n_z)
    z_peer = lambda k: (dp, chip(k) * 2 + core)
    dp_peer = lambda k: (lax.rem(dp + k, n_dp), ctx)
    ctx_peer = lambda k: (dp, lax.rem(ctx + k, n_ctx))
    greet([ctx_peer(k) for k in range(1, n_ctx)] + [dp_peer(k) for k in range(1, n_dp)])
    order = list(range(1, n_z)) + [0]
    pending = []

    def send(src, dst, s, r, peer):
        copy = remote(src, dst, s, r, peer)
        copy.start()
        pending.append(copy)
        return copy

    def term_rows(index):
        return pl.ds(pl.multiple_of(index * tokens, tokens), tokens)

    first = {}
    for k in order:
        first[k] = send(
            term_ref.at[term_rows(chip(k) * 2 + other)], pair_in.at[k], a_send.at[k], a_recv.at[k], partner
        )
    second = {}
    mine = None
    for k in order:
        first[k].wait_recv()
        added = term_ref[term_rows(chip(k) * 2 + core), :].astype(wide) + pair_in[k].astype(wide)
        if k == 0:
            mine = added
        else:
            pair_sum[k] = added.astype(low)
            second[k] = send(pair_sum.at[k], z_in.at[k], b_send.at[k], b_recv.at[k], z_peer(k))
    batch = layer_ref.shape[0]
    for d in range(batch):
        turned[:, d * tokens : (d + 1) * tokens] = layer_ref[d].T
    for k in range(1, n_z):
        second[k].wait_recv()
        mine = mine + z_in[k].astype(wide)
    joined_ref[...] = mine.astype(low)
    blocks_in[dp] = mine.astype(low)

    third = []
    for k in range(1, n_dp):
        third.append(send(joined_ref, blocks_in.at[dp], c_send.at[k], c_recv.at[k], dp_peer(k)))
    values = []
    for k in range(1, n_ctx):
        values.append(
            send(
                value_ref.at[lax.rem(ctx + k, n_ctx)], value_in.at[k], d_send.at[k], d_recv.at[k], ctx_peer(k)
            )
        )
    for copy in third:
        copy.wait_recv()
    every = blocks_in[...].reshape(batch * tokens, blocks_in.shape[2])

    height = down_ref.shape[0]

    def turned_rows(index):
        return turned[pl.ds(pl.multiple_of(index * height, 16), height), :]

    fourth = {}
    for k in order:
        down_out[k] = dot(turned_rows(chip(k) * 2 + other), every, 1, 0).astype(low)
        fourth[k] = send(down_out.at[k], down_in.at[k], e_send.at[k], e_recv.at[k], partner)
    fifth = {}
    own = None
    for k in order:
        part = dot(turned_rows(chip(k) * 2 + core), every, 1, 0)
        fourth[k].wait_recv()
        part = part + down_in[k].astype(wide)
        if k == 0:
            down_own[...] = part
        else:
            down_sum[k] = part.astype(low)
            fifth[k] = send(down_sum.at[k], down_z.at[k], f_send.at[k], f_recv.at[k], z_peer(k))
    value = value_ref[ctx].astype(wide)
    for k in range(1, n_ctx):
        values[k - 1].wait_recv()
        value = value + value_in[k].astype(wide)
    uv_ref[...] = value
    for k in range(1, n_z):
        fifth[k].wait_recv()
        down_own[...] += down_z[k].astype(wide)
    down_ref[...] = down_own[...]
    for copy in pending:
        copy.wait_send()


def body(n_dp, n_ctx, layer_input, kv_latent, key_rope, q_latent, q_rope, saved_output, w_uv, d_out, blocks):
    tokens = kv_latent.shape[1]
    half_rows = tokens // 2
    heads, latent = q_latent.shape[2], q_latent.shape[3]
    rope_width = key_rope.shape[2]
    width = latent + rope_width
    value_width = w_uv.shape[1] // heads
    seq_rows = half_rows * blocks.shape[0]
    rows = tokens * heads
    n_z = n_ctx // 2
    values = w_uv.shape[1]
    vmem = pl.BlockSpec(memory_space=pltpu.VMEM)
    dma = lambda n: pltpu.SemaphoreType.DMA((n,))

    keys = jnp.concatenate([kv_latent[0], key_rope[0]], axis=1)
    head_of = jnp.arange(values, dtype=jnp.int32) // value_width
    keep = head_of[None, :] == jnp.arange(heads, dtype=jnp.int32)[:, None]
    spread = jnp.where(keep[None], d_out[0][:, None, :], jnp.zeros((), low)).reshape(rows, values)
    saved = saved_output[0].reshape(rows, latent)
    offsets = jnp.arange(half_rows, dtype=jnp.int32)
    pos_key = (blocks[:, None] * half_rows + offsets[None, :]).reshape(seq_rows, 1)
    own_blocks = lax.dynamic_slice_in_dim(blocks, 2 * lax.axis_index("ctx"), 2, 0)
    pos_query = jnp.repeat(
        (own_blocks[:, None] * half_rows + offsets[None, :]).reshape(tokens), heads
    ).reshape(1, rows)

    all_keys, grad, delta, value_sum = pl.pallas_call(
        functools.partial(gather_kernel, n_dp, n_ctx),
        out_shape=(
            jax.ShapeDtypeStruct((seq_rows, width), low),
            jax.ShapeDtypeStruct((rows, latent), low),
            jax.ShapeDtypeStruct((1, rows), wide),
            jax.ShapeDtypeStruct((n_ctx, latent // (n_dp * n_ctx), values), low),
        ),
        in_specs=[vmem] * 4,
        out_specs=(vmem,) * 4,
        scratch_shapes=[
            pltpu.VMEM((n_dp, latent // n_dp, values), low),
            pltpu.VMEM((n_dp, latent // n_dp, values), low),
            dma(n_z), dma(n_z), dma(n_z), dma(n_z), dma(n_dp), dma(n_dp),
        ],
        compiler_params=pltpu.CompilerParams(
            collective_id=0, has_side_effects=True, vmem_limit_bytes=VMEM_LIMIT
        ),
        name="gather",
    )(keys, spread, w_uv, saved)

    tile = min(256, rows)
    whole = lambda shape: pl.BlockSpec(shape, lambda i: (0, 0))
    d_lat, d_rope, term = pl.pallas_call(
        attend_kernel,
        grid=(rows // tile,),
        out_shape=(
            jax.ShapeDtypeStruct((rows, latent), low),
            jax.ShapeDtypeStruct((rows, rope_width), low),
            jax.ShapeDtypeStruct((seq_rows, width), low),
        ),
        in_specs=[
            whole((seq_rows, width)),
            whole((seq_rows, 1)),
            pl.BlockSpec((1, tile), lambda i: (0, i)),
            pl.BlockSpec((1, tile), lambda i: (0, i)),
            pl.BlockSpec((tile, latent), lambda i: (i, 0)),
            pl.BlockSpec((tile, rope_width), lambda i: (i, 0)),
            pl.BlockSpec((tile, latent), lambda i: (i, 0)),
        ],
        out_specs=(
            pl.BlockSpec((tile, latent), lambda i: (i, 0)),
            pl.BlockSpec((tile, rope_width), lambda i: (i, 0)),
            whole((seq_rows, width)),
        ),
        scratch_shapes=[pltpu.VMEM((seq_rows, width), wide)],
        compiler_params=pltpu.CompilerParams(
            dimension_semantics=("arbitrary",), vmem_limit_bytes=VMEM_LIMIT
        ),
        name="attend",
    )(
        all_keys, pos_key, pos_query, delta,
        q_latent[0].reshape(rows, latent), q_rope[0].reshape(rows, rope_width), grad,
    )

    height = layer_input.shape[2] // n_ctx
    batch = layer_input.shape[0]
    joined, grad_down, grad_uv = pl.pallas_call(
        functools.partial(reduce_kernel, n_dp, n_ctx),
        out_shape=(
            jax.ShapeDtypeStruct((tokens, width), low),
            jax.ShapeDtypeStruct((height, width), wide),
            jax.ShapeDtypeStruct((latent // (n_dp * n_ctx), values), wide),
        ),
        in_specs=[vmem] * 3,
        out_specs=(vmem,) * 3,
        scratch_shapes=[
            pltpu.VMEM((layer_input.shape[2], batch * tokens), low),
            pltpu.VMEM((n_z, tokens, width), low),
            pltpu.VMEM((n_z, tokens, width), low),
            pltpu.VMEM((n_z, tokens, width), low),
            pltpu.VMEM((n_dp, tokens, width), low),
            pltpu.VMEM((n_z, height, width), low),
            pltpu.VMEM((height, width), wide),
            pltpu.VMEM((n_z, height, width), low),
            pltpu.VMEM((n_z, height, width), low),
            pltpu.VMEM((n_z, height, width), low),
            pltpu.VMEM((n_ctx, latent // (n_dp * n_ctx), values), low),
            dma(n_z), dma(n_z), dma(n_z), dma(n_z), dma(n_dp), dma(n_dp),
            dma(n_ctx), dma(n_ctx), dma(n_z), dma(n_z), dma(n_z), dma(n_z),
        ],
        compiler_params=pltpu.CompilerParams(
            collective_id=1, has_side_effects=True, vmem_limit_bytes=VMEM_LIMIT
        ),
        name="reduce",
    )(term, layer_input, value_sum)
    return (
        d_lat.reshape(1, tokens, heads, latent),
        d_rope.reshape(1, tokens, heads, rope_width),
        joined[None, :, :latent],
        joined[None, :, latent:],
        grad_down,
        grad_uv,
    )


def solution(mesh):
    n_dp, n_ctx = mesh.shape["dp"], mesh.shape["ctx"]
    in_specs = (
        P(None, "ctx", "dp"),
        P("dp", "ctx", None),
        P("dp", "ctx", None),
        P("dp", "ctx", None, None),
        P("dp", "ctx", None, None),
        P("dp", "ctx", None, None),
        P(),
        P("dp", "ctx", None),
        P(),
    )
    out_specs = (
        P("dp", "ctx", None, None),
        P("dp", "ctx", None, None),
        P("dp", "ctx", None),
        P("dp", "ctx", None),
        P(("dp", "ctx"), None),
        P(("dp", "ctx"), None),
    )
    return jax.shard_map(
        functools.partial(body, n_dp, n_ctx),
        mesh=mesh, in_specs=in_specs, out_specs=out_specs, check_vma=False,
    )
```

```python
import functools
import math

import jax
import jax.numpy as jnp
from jax import lax
from jax.experimental import pallas as pl
from jax.experimental.pallas import tpu as pltpu
from jax.sharding import PartitionSpec as P

softmax_scale = 1.0 / math.sqrt(192.0)
wide = jnp.float32
low = jnp.bfloat16
MESH = pl.DeviceIdType.MESH
VMEM_LIMIT = 62 * 1024 * 1024


def dot(a, b, ca, cb):
    return lax.dot_general(a, b, (((ca,), (cb,)), ((), ())), preferred_element_type=wide)


def greet(peers):
    barrier = pltpu.get_barrier_semaphore()
    for peer in peers:
        pl.semaphore_signal(barrier, inc=1, device_id=peer, device_id_type=MESH)
    pl.semaphore_wait(barrier, len(peers))


def remote(src, dst, send, recv, peer):
    return pltpu.make_async_remote_copy(
        src_ref=src, dst_ref=dst, send_sem=send, recv_sem=recv, device_id=peer, device_id_type=MESH
    )


def gather_kernel(
    n_dp, n_ctx,
    lat_ref, rope_ref, out_ref, weight_ref, saved_ref,
    keys_ref, grad_ref, delta_ref, value_ref,
    key_ref, spread_ref, parts, landed, key_send, key_recv, pair_send, pair_recv, val_send, val_recv,
):
    dp, ctx = lax.axis_index("dp"), lax.axis_index("ctx")
    n_z = n_ctx // 2
    z, core = ctx // 2, ctx % 2
    tokens, latent = lat_ref.shape
    partner = (dp, z * 2 + (1 - core))
    key_ref[:, :latent] = lat_ref[...]
    key_ref[:, latent:] = rope_ref[...]
    z_peer = lambda k: (dp, lax.rem(z + k, n_z) * 2 + core)
    dp_peer = lambda k: (lax.rem(dp + k, n_dp), ctx)
    greet(
        [partner]
        + [z_peer(k) for k in range(1, n_z)]
        + [dp_peer(k) for k in range(1, n_dp)]
    )

    def rows_of(index):
        return keys_ref.at[pl.ds(pl.multiple_of(index * tokens, tokens), tokens)]

    sends = []
    for k in range(1, n_z):
        copy = remote(key_ref, rows_of(ctx), key_send.at[k], key_recv.at[k], z_peer(k))
        copy.start()
        sends.append(copy)
    pair = remote(key_ref, rows_of(ctx), pair_send.at[0], pair_recv.at[0], partner)
    pair.start()
    keys_ref[pl.ds(pl.multiple_of(ctx * tokens, tokens), tokens), :] = key_ref[...]

    heads = spread_ref.shape[0] // tokens
    values = out_ref.shape[1]
    lane = lax.broadcasted_iota(jnp.int32, (heads, values), 1)
    head = lax.broadcasted_iota(jnp.int32, (heads, values), 0)
    keep = (lane // (values // heads) == head)[None]
    group = min(16, tokens)
    for start in range(0, tokens, group):
        piece = out_ref[start : start + group].astype(wide)
        piece = jnp.broadcast_to(piece[:, None, :], (group, heads, values))
        piece = jnp.where(keep, piece, 0.0).reshape(group * heads, values)
        spread_ref[start * heads : (start + group) * heads, :] = piece.astype(low)

    share = parts.shape[1]
    value = dot(saved_ref[...], spread_ref[...], 0, 0).astype(low)
    for d in range(n_dp):
        parts[d] = value[d * share : (d + 1) * share]
    value_copies = []
    for k in range(1, n_dp):
        copy = remote(
            parts.at[lax.rem(dp + k, n_dp)], landed.at[k], val_send.at[k], val_recv.at[k], dp_peer(k)
        )
        copy.start()
        value_copies.append(copy)

    rows = spread_ref.shape[0]
    tile = min(256, rows)
    for start in range(0, rows, tile):
        grad = dot(spread_ref[start : start + tile], weight_ref[...], 1, 1).astype(low)
        grad_ref[start : start + tile, :] = grad
        prod = grad.astype(wide) * saved_ref[start : start + tile].astype(wide)
        part = prod[:, :128]
        for lane in range(128, prod.shape[1], 128):
            part = part + prod[:, lane : lane + 128]
        delta_ref[:, start : start + tile] = jnp.sum(part.T, axis=0, keepdims=True)

    passes = []
    for k in range(1, n_z):
        owner = lax.rem(z + n_z - k, n_z) * 2 + core
        remote(key_ref, rows_of(owner), key_send.at[k], key_recv.at[k], z_peer(k)).wait_recv()
        copy = remote(rows_of(owner), rows_of(owner), pair_send.at[k], pair_recv.at[k], partner)
        copy.start()
        passes.append(copy)
    total = parts[dp].astype(wide)
    for k in range(1, n_dp):
        value_copies[k - 1].wait_recv()
        total = total + landed[k].astype(wide)
    total = total.astype(low)
    piece = value_ref.shape[1]
    for c in range(n_ctx):
        value_ref[c] = total[c * piece : (c + 1) * piece]
    for k in range(n_z):
        owner = lax.rem(z + n_z - k, n_z) * 2 + (1 - core)
        remote(rows_of(owner), rows_of(owner), pair_send.at[k], pair_recv.at[k], partner).wait_recv()
    for copy in sends + [pair] + passes + value_copies:
        copy.wait_send()


def reduce_kernel(
    n_dp, n_ctx,
    blocks_ref, keys_ref, delta_ref, ql_ref, qr_ref, grad_ref, layer_ref, value_ref,
    dql_ref, dqr_ref, joined_ref, down_ref, uv_ref,
    posk, probs_all, slopes, chip_part, term_out,
    turned, pair_in, pair_sum, z_in, blocks_in, down_out, down_own, down_in, down_sum, down_z, value_in,
    a_send, a_recv, b_send, b_recv, c_send, c_recv, d_send, d_recv, e_send, e_recv, f_send, f_recv,
):
    dp, ctx = lax.axis_index("dp"), lax.axis_index("ctx")
    n_z = n_ctx // 2
    z, core = ctx // 2, ctx % 2
    tokens = joined_ref.shape[0]
    other = 1 - core
    partner = (dp, z * 2 + other)
    chip = lambda k: lax.rem(z + k, n_z)
    z_peer = lambda k: (dp, chip(k) * 2 + core)
    dp_peer = lambda k: (lax.rem(dp + k, n_dp), ctx)
    ctx_peer = lambda k: (dp, lax.rem(ctx + k, n_ctx))
    greet([ctx_peer(k) for k in range(1, n_ctx)] + [dp_peer(k) for k in range(1, n_dp)])
    order = list(range(1, n_z)) + [0]
    pending = []

    def send(src, dst, s, r, peer):
        copy = remote(src, dst, s, r, peer)
        copy.start()
        pending.append(copy)
        return copy

    seq_rows = keys_ref.shape[0]
    rows, latent = ql_ref.shape
    heads = rows // tokens
    half = tokens // 2
    tile = min(256, rows)
    for j in range(seq_rows // half):
        posk[j * half : (j + 1) * half, :] = blocks_ref[j] * half + lax.broadcasted_iota(
            jnp.int32, (half, 1), 0
        )
    low_block, high_block = blocks_ref[2 * ctx], blocks_ref[2 * ctx + 1]

    def score_tile(i, carry):
        span = pl.ds(pl.multiple_of(i * tile, tile), tile)
        token = (i * tile + lax.broadcasted_iota(jnp.int32, (1, tile), 1)) // heads
        posq = jnp.where(token < half, low_block * half + token, high_block * half + token - half)
        key_lat, key_rope = keys_ref[:, :latent], keys_ref[:, latent:]
        scores = dot(key_lat, ql_ref[span, :], 1, 1) + dot(key_rope, qr_ref[span, :], 1, 1)
        scores = jnp.where(posk[...] <= posq, scores * softmax_scale, -jnp.inf)
        expo = jnp.exp(scores - jnp.max(scores, axis=0, keepdims=True))
        probs = expo * (1.0 / jnp.sum(expo, axis=0, keepdims=True))
        grad_prob = dot(key_lat, grad_ref[span, :], 1, 1)
        probs_all[:, span] = probs.astype(low)
        slopes[:, span] = (probs * (grad_prob - delta_ref[:, span])).astype(low)
        return carry

    lax.fori_loop(0, rows // tile, score_tile, 0)

    first, second = {}, {}

    def finish(at):
        k, slot = order[at], at % 2
        first[k].wait_recv()
        added = chip_part[slot, pl.ds(pl.multiple_of(core * tokens, tokens), tokens), :] + pair_in[k].astype(wide)
        if k == 0:
            return added
        pair_sum[k] = added.astype(low)
        second[k] = send(pair_sum.at[k], z_in.at[k], b_send.at[k], b_recv.at[k], z_peer(k))

    for at, k in enumerate(order):
        span = pl.ds(pl.multiple_of(chip(k) * (2 * tokens), 2 * tokens), 2 * tokens)
        slope = slopes[span, :]
        slot = at % 2
        chip_part[slot, :, :latent] = dot(probs_all[span, :], grad_ref[...], 1, 0) + softmax_scale * dot(
            slope, ql_ref[...], 1, 0
        )
        chip_part[slot, :, latent:] = softmax_scale * dot(slope, qr_ref[...], 1, 0)
        term_out[k] = chip_part[slot, pl.ds(pl.multiple_of(other * tokens, tokens), tokens), :].astype(low)
        first[k] = send(term_out.at[k], pair_in.at[k], a_send.at[k], a_recv.at[k], partner)
        if at > 0:
            finish(at - 1)
    mine = finish(n_z - 1)

    def query_tile(i, carry):
        span = pl.ds(pl.multiple_of(i * tile, tile), tile)
        slope = slopes[:, span]
        dql_ref[span, :] = (softmax_scale * dot(slope, keys_ref[:, :latent], 0, 0)).astype(low)
        dqr_ref[span, :] = (softmax_scale * dot(slope, keys_ref[:, latent:], 0, 0)).astype(low)
        return carry

    lax.fori_loop(0, rows // tile, query_tile, 0)
    batch = layer_ref.shape[0]
    for d in range(batch):
        turned[:, d * tokens : (d + 1) * tokens] = layer_ref[d].T
    for k in range(1, n_z):
        second[k].wait_recv()
        mine = mine + z_in[k].astype(wide)
    joined_ref[...] = mine.astype(low)
    blocks_in[dp] = mine.astype(low)

    third = []
    for k in range(1, n_dp):
        third.append(send(joined_ref, blocks_in.at[dp], c_send.at[k], c_recv.at[k], dp_peer(k)))
    values = []
    for k in range(1, n_ctx):
        values.append(
            send(
                value_ref.at[lax.rem(ctx + k, n_ctx)], value_in.at[k], d_send.at[k], d_recv.at[k], ctx_peer(k)
            )
        )
    for copy in third:
        copy.wait_recv()
    every = blocks_in[...].reshape(batch * tokens, blocks_in.shape[2])

    height = down_ref.shape[0]

    def turned_rows(index):
        return turned[pl.ds(pl.multiple_of(index * height, 16), height), :]

    fourth = {}
    for k in order:
        down_out[k] = dot(turned_rows(chip(k) * 2 + other), every, 1, 0).astype(low)
        fourth[k] = send(down_out.at[k], down_in.at[k], e_send.at[k], e_recv.at[k], partner)
    fifth = {}
    own = None
    for k in order:
        part = dot(turned_rows(chip(k) * 2 + core), every, 1, 0)
        fourth[k].wait_recv()
        part = part + down_in[k].astype(wide)
        if k == 0:
            down_own[...] = part
        else:
            down_sum[k] = part.astype(low)
            fifth[k] = send(down_sum.at[k], down_z.at[k], f_send.at[k], f_recv.at[k], z_peer(k))
    value = value_ref[ctx].astype(wide)
    for k in range(1, n_ctx):
        values[k - 1].wait_recv()
        value = value + value_in[k].astype(wide)
    uv_ref[...] = value
    for k in range(1, n_z):
        fifth[k].wait_recv()
        down_own[...] += down_z[k].astype(wide)
    down_ref[...] = down_own[...]
    for copy in pending:
        copy.wait_send()


def body(n_dp, n_ctx, layer_input, kv_latent, key_rope, q_latent, q_rope, saved_output, w_uv, d_out, blocks):
    tokens = kv_latent.shape[1]
    half_rows = tokens // 2
    heads, latent = q_latent.shape[2], q_latent.shape[3]
    rope_width = key_rope.shape[2]
    width = latent + rope_width
    seq_rows = half_rows * blocks.shape[0]
    rows = tokens * heads
    n_z = n_ctx // 2
    values = w_uv.shape[1]
    vmem = pl.BlockSpec(memory_space=pltpu.VMEM)
    dma = lambda n: pltpu.SemaphoreType.DMA((n,))

    saved = saved_output[0].reshape(rows, latent)
    all_keys, grad, delta, value_sum = pl.pallas_call(
        functools.partial(gather_kernel, n_dp, n_ctx),
        out_shape=(
            jax.ShapeDtypeStruct((seq_rows, width), low),
            jax.ShapeDtypeStruct((rows, latent), low),
            jax.ShapeDtypeStruct((1, rows), wide),
            jax.ShapeDtypeStruct((n_ctx, latent // (n_dp * n_ctx), values), low),
        ),
        in_specs=[vmem] * 5,
        out_specs=(vmem,) * 4,
        scratch_shapes=[
            pltpu.VMEM((tokens, width), low),
            pltpu.VMEM((rows, values), low),
            pltpu.VMEM((n_dp, latent // n_dp, values), low),
            pltpu.VMEM((n_dp, latent // n_dp, values), low),
            dma(n_z), dma(n_z), dma(n_z), dma(n_z), dma(n_dp), dma(n_dp),
        ],
        compiler_params=pltpu.CompilerParams(
            collective_id=0, has_side_effects=True, vmem_limit_bytes=VMEM_LIMIT
        ),
        name="gather",
    )(kv_latent[0], key_rope[0], d_out[0], w_uv, saved)

    height = layer_input.shape[2] // n_ctx
    batch = layer_input.shape[0]
    d_lat, d_rope, joined, grad_down, grad_uv = pl.pallas_call(
        functools.partial(reduce_kernel, n_dp, n_ctx),
        out_shape=(
            jax.ShapeDtypeStruct((rows, latent), low),
            jax.ShapeDtypeStruct((rows, rope_width), low),
            jax.ShapeDtypeStruct((tokens, width), low),
            jax.ShapeDtypeStruct((height, width), wide),
            jax.ShapeDtypeStruct((latent // (n_dp * n_ctx), values), wide),
        ),
        in_specs=[pl.BlockSpec(memory_space=pltpu.SMEM)] + [vmem] * 7,
        out_specs=(vmem,) * 5,
        scratch_shapes=[
            pltpu.VMEM((seq_rows, 1), jnp.int32),
            pltpu.VMEM((seq_rows, rows), low),
            pltpu.VMEM((seq_rows, rows), low),
            pltpu.VMEM((2, 2 * tokens, width), wide),
            pltpu.VMEM((n_z, tokens, width), low),
            pltpu.VMEM((layer_input.shape[2], batch * tokens), low),
            pltpu.VMEM((n_z, tokens, width), low),
            pltpu.VMEM((n_z, tokens, width), low),
            pltpu.VMEM((n_z, tokens, width), low),
            pltpu.VMEM((n_dp, tokens, width), low),
            pltpu.VMEM((n_z, height, width), low),
            pltpu.VMEM((height, width), wide),
            pltpu.VMEM((n_z, height, width), low),
            pltpu.VMEM((n_z, height, width), low),
            pltpu.VMEM((n_z, height, width), low),
            pltpu.VMEM((n_ctx, latent // (n_dp * n_ctx), values), low),
            dma(n_z), dma(n_z), dma(n_z), dma(n_z), dma(n_dp), dma(n_dp),
            dma(n_ctx), dma(n_ctx), dma(n_z), dma(n_z), dma(n_z), dma(n_z),
        ],
        compiler_params=pltpu.CompilerParams(
            collective_id=1, has_side_effects=True, vmem_limit_bytes=VMEM_LIMIT
        ),
        name="reduce",
    )(
        blocks, all_keys, delta,
        q_latent[0].reshape(rows, latent), q_rope[0].reshape(rows, rope_width),
        grad, layer_input, value_sum,
    )
    return (
        d_lat.reshape(1, tokens, heads, latent),
        d_rope.reshape(1, tokens, heads, rope_width),
        joined[None, :, :latent],
        joined[None, :, latent:],
        grad_down,
        grad_uv,
    )


def solution(mesh):
    n_dp, n_ctx = mesh.shape["dp"], mesh.shape["ctx"]
    in_specs = (
        P(None, "ctx", "dp"),
        P("dp", "ctx", None),
        P("dp", "ctx", None),
        P("dp", "ctx", None, None),
        P("dp", "ctx", None, None),
        P("dp", "ctx", None, None),
        P(),
        P("dp", "ctx", None),
        P(),
    )
    out_specs = (
        P("dp", "ctx", None, None),
        P("dp", "ctx", None, None),
        P("dp", "ctx", None),
        P("dp", "ctx", None),
        P(("dp", "ctx"), None),
        P(("dp", "ctx"), None),
    )
    return jax.shard_map(
        functools.partial(body, n_dp, n_ctx),
        mesh=mesh, in_specs=in_specs, out_specs=out_specs, check_vma=False,
    )
```
